32 devices in a mesh: dp: 8 (over z, y), grp: 4 (over x, core).
Axes of the slice: x: 2, y: 2, z: 4, core: 2. Of those that a mesh axis runs over, the one named last changes fastest.
Arguments:
- quot_ids: int32 [4096, 2], P(('dp', 'grp')), may hold values from 0 to 127
- rem_ids: int32 [4096, 2], P(('dp', 'grp')), may hold values from 0 to 16383, as said below
- labels: int32 [4096], P(('dp', 'grp')), may hold values 0 or 1
- quot_table: bfloat16 [2, 128, 512], replicated, may hold values from -6 to 6
- rem_table: bfloat16 [2, 16384, 512], P(None, 'grp'), may hold values from -6 to 6
- w1: bfloat16 [1024, 512], replicated, may hold values from -0.1875 to 0.1875
- b1: float32 [512], replicated, may hold values from -3 to 3
- w2: bfloat16 [512], replicated, may hold values from -0.5 to 0.5
- b2: float32 [1], replicated, may hold values from -3 to 3
Outputs:
- losses: float32 [4096], P(('dp', 'grp'))
- grad_rem: float32 [2, 16384, 512], P(None, 'grp', 'dp')
- grad_quot: float32 [2, 128, 512], replicated
- grad_w1: float32 [1024, 512], replicated
- grad_b1: float32 [512], replicated
- grad_w2: float32 [512], replicated
- grad_b2: float32 [1], replicated
The draws below stay inside these ranges and needn't reach their ends.
Inputs may be any that keep to these rules, and one draw needn't show every extreme that they name: `rem_ids`: in each aligned block of 128 samples and each feature, at most 64 remainder indices r share the same r // 4096, and exactly 64 do for some value of r // 4096.
All inputs are finite; a program needn't handle non-finite values. No bound on the sum of `labels` on one device may be relied on, other than what follows from the above.
Results may differ from the reference program's by a relative error of at most 0.0051.
Values may be sent and summed in bfloat16 or wider, within the bound.
No kernel may reach another device: no remote copies, remote signals or barrier semaphores. Data moves between devices by JAX's collectives and lax.ppermute only.
A program may use at most 128 MiB of HBM per device.

```python
import jax
import jax.numpy as jnp
from jax import lax

D = 512
HID = 512
QROWS = 128
REM_DEV = 4096
FEAT = 2
TOK_DEV = 128
REM = 16384
TOKENS = 4096
CAP = 64
N_GRP = 4


def draw_rem_ids(key, part):
    blocks = TOKENS // TOK_DEV
    spare = N_GRP * CAP - CAP

    def draw_block(block_key):
        key_hot, key_pool, key_order, key_inner = jax.random.split(block_key, 4)
        hottest = jax.random.randint(key_hot, (), 0, N_GRP)
        others = (jnp.arange(spare, dtype=jnp.int32) // CAP + 1 + hottest) % N_GRP
        pool = jnp.concatenate([jnp.full((CAP,), hottest, jnp.int32), others.astype(jnp.int32)])
        order = jnp.concatenate([jnp.arange(CAP, dtype=jnp.int32), CAP + jax.random.permutation(key_pool, spare).astype(jnp.int32)])[:TOK_DEV]
        owners = pool[order]
        owners = owners[jax.random.permutation(key_order, TOK_DEV)]
        inner_rows = jax.random.randint(key_inner, (TOK_DEV,), 0, REM_DEV)
        return (owners * REM_DEV + inner_rows).astype(jnp.int32)
    block_keys = jax.random.split(jax.random.fold_in(key, 17), blocks * FEAT)
    values = jax.vmap(draw_block)(block_keys)
    return values.reshape(blocks, FEAT, TOK_DEV).transpose(0, 2, 1).reshape(TOKENS, FEAT)


def place_ends(entries, own_key, least, high):
    extent = entries.shape
    place = [jax.random.randint(jax.random.fold_in(own_key, axis), (), 0, extent[axis]) for axis in range(len(extent))]
    entries = entries.at[tuple(place)].set(least)
    longest = extent.index(max(extent))
    place[longest] = (place[longest] + 1) % extent[longest]
    return entries.at[tuple(place)].set(high)


def steps_of(key, dims, shards, smallest, largest):
    loudness, own = 1.0, jax.random.fold_in(key, 6)
    for position, shards_of in shards:
        steps = jnp.exp(jax.random.uniform(jax.random.fold_in(own, position), (shards_of,), jnp.float32, smallest / len(shards), largest / len(shards)))
        loudness = loudness * jnp.repeat(steps, dims[position] // shards_of).reshape([-1 if axis == position else 1 for axis in range(len(dims))])
    return loudness


def centred(stream_key, extent, width, bound, shards=(), kind=jnp.bfloat16):
    result = width * jax.random.normal(stream_key, extent, jnp.float32)
    if shards:
        result = result * steps_of(stream_key, extent, shards, -0.22, 0.18)
    return jnp.clip(result, -bound, bound).astype(kind)


def setup_inputs(seed: int = 0) -> dict:
    seeds = jax.random.split(jax.random.key(seed), 10)
    quot_ids = place_ends(jax.random.randint(seeds[0], (TOKENS, FEAT), 0, QROWS), jax.random.fold_in(seeds[0], 1), 0, QROWS - 1).astype(jnp.int32)
    rem_ids = draw_rem_ids(jax.random.fold_in(seeds[9], 71), 0)
    labels = place_ends((jax.random.randint(seeds[2], (TOKENS,), 0, 2) < 1).astype(jnp.int32), jax.random.fold_in(seeds[2], 1), 0, 1)
    quot_table = centred(seeds[3], (FEAT, QROWS, D), 1.0, 6.0)
    rem_table = centred(seeds[4], (FEAT, REM, D), 1.0, 6.0, ((1, 4),))
    w1 = centred(seeds[5], (FEAT * D, HID), (FEAT * D) ** -0.5, 0.1875)
    b1 = centred(seeds[6], (HID,), 0.5, 3.0, (), jnp.float32)
    w2 = centred(seeds[7], (HID,), (HID // 4) ** -0.5, 0.5)
    b2 = centred(seeds[8], (1,), 1.0, 3.0, (), jnp.float32)
    return dict(quot_ids=quot_ids, rem_ids=rem_ids, labels=labels, quot_table=quot_table, rem_table=rem_table, w1=w1, b1=b1, w2=w2, b2=b2)


def reference(quot_ids, rem_ids, labels, quot_table, rem_table, w1, b1, w2, b2):
    quot_parts = []
    rem_parts = []
    onehots = []
    for feature in range(FEAT):
        onehot = (quot_ids[:, feature][:, None] == jnp.arange(QROWS, dtype=jnp.int32)[None, :]).astype(jnp.bfloat16)
        onehots.append(onehot)
        quot_parts.append(jnp.dot(onehot, quot_table[feature], preferred_element_type=jnp.float32))
        rem_parts.append(jnp.take(rem_table[feature], rem_ids[:, feature], axis=0).astype(jnp.float32))
    quot_rows = jnp.concatenate(quot_parts, axis=1)
    rem_rows = jnp.concatenate(rem_parts, axis=1)
    joined = (quot_rows * rem_rows).astype(jnp.bfloat16)
    preact = jnp.dot(joined, w1, preferred_element_type=jnp.float32) + b1
    hidden = jax.nn.silu(preact).astype(jnp.bfloat16)
    logits = jnp.dot(hidden, w2, preferred_element_type=jnp.float32) + b2[0]
    target = labels.astype(jnp.float32)
    losses = jax.nn.softplus(logits) - target * logits
    dlogits = jax.nn.sigmoid(logits) - target
    grad_b2 = jnp.sum(dlogits)[None]
    grad_w2 = jnp.dot(dlogits, hidden.astype(jnp.float32), precision=lax.Precision.HIGHEST)
    sigmoid_pre = jax.nn.sigmoid(preact)
    slopes = sigmoid_pre * (1.0 + preact * (1.0 - sigmoid_pre))
    dpreact = dlogits[:, None] * w2.astype(jnp.float32)[None, :] * slopes
    grad_b1 = jnp.sum(dpreact, axis=0)
    rounded = dpreact.astype(jnp.bfloat16)
    grad_w1 = jnp.dot(joined.T, rounded, preferred_element_type=jnp.float32)
    djoined = jnp.dot(rounded, w1.T, preferred_element_type=jnp.float32)
    rem_grads = (djoined * quot_rows).astype(jnp.bfloat16)
    quot_grads = djoined * rem_rows
    grad_rem = jnp.zeros((FEAT, REM, D), jnp.float32)
    quot_list = []
    for feature in range(FEAT):
        grad_block = rem_grads[:, feature * D:(feature + 1) * D].astype(jnp.float32)
        grad_rem = grad_rem.at[feature, rem_ids[:, feature]].add(grad_block)
        quot_list.append(jnp.dot(onehots[feature].astype(jnp.float32).T, quot_grads[:, feature * D:(feature + 1) * D], precision=lax.Precision.HIGHEST))
    grad_quot = jnp.stack(quot_list, axis=0)
    return losses, grad_rem, grad_quot, grad_w1, grad_b1, grad_w2, grad_b2
```

```python
import functools

import jax
import jax.numpy as jnp
from jax import lax
from jax.experimental import pallas as pl
from jax.experimental.pallas import tpu as pltpu
from jax.sharding import Mesh, PartitionSpec as P


f32 = jnp.float32
bf16 = jnp.bfloat16
VM = pl.BlockSpec(memory_space=pltpu.VMEM)
SM = pl.BlockSpec(memory_space=pltpu.SMEM)
TINY = 8
HIGH = 256


def iota(shape, dim):
    return lax.broadcasted_iota(jnp.int32, shape, dim)


def mm(a, b, dims=((1,), (0,)), **kw):
    return lax.dot_general(a, b, (dims, ((), ())), preferred_element_type=f32, **kw)


def call(body, outs, args, in_specs, scratch=()):
    multi = isinstance(outs, (tuple, list))
    return pl.pallas_call(
        body,
        out_shape=outs,
        in_specs=in_specs,
        out_specs=tuple(VM for _ in outs) if multi else VM,
        scratch_shapes=list(scratch),
    )(*args)


def tree_sum(parts):
    parts = list(parts)
    while len(parts) > 1:
        parts = [a + b for a, b in zip(parts[::2], parts[1::2])]
    return parts[0]


def pack_tiny(b1_row, w2_row, b2_row):
    width = b1_row.shape[1]
    which = iota((TINY, width), 0)
    out = jnp.zeros((TINY, width), f32)
    at = 0
    for row in (b1_row, w2_row, b2_row):
        rest = row
        for _ in range(3):
            head = rest.astype(bf16).astype(f32)
            if at < TINY:
                out = jnp.where(which == at, head, out)
            rest = rest - head
            at += 1
        if at == 6:
            break
    lane = iota((1, width), 1)
    rest = b2_row
    last = jnp.zeros((1, width), f32)
    for piece in range(3):
        head = rest.astype(bf16).astype(f32)
        last = jnp.where(lane == piece, head, last)
        rest = rest - head
    out = jnp.where(which == 6, last, out)
    return out.astype(bf16)


def unpack_tiny(block):
    block = block.astype(f32)
    b1_row = block[0:1] + block[1:2] + block[2:3]
    w2_row = block[3:4] + block[4:5] + block[5:6]
    b2_row = block[6:7, 0:1] + block[6:7, 1:2] + block[6:7, 2:3]
    return b1_row, w2_row, jnp.broadcast_to(b2_row, b1_row.shape)


def fetch_body(me_ref, ids_ref, table_ref, out_ref, *, cap):
    n_rows, tok = ids_ref.shape
    feats, shard, _ = table_ref.shape
    groups = n_rows // feats
    local = ids_ref[...] - me_ref[0] * shard
    mine = (local >= 0) & (local < shard)
    before = (iota((tok, tok), 0) < iota((tok, tok), 1)).astype(f32)
    key = jnp.where(mine, mm(mine.astype(f32), before), -1.0).astype(jnp.int32)
    value = local.astype(f32)
    slot = iota((cap, tok), 0)
    for f in range(feats):
        cols = []
        for k in range(groups):
            at = slice(k * feats + f, k * feats + f + 1)
            hit = jnp.where(key[at, :] == slot, value[at, :], 0.0)
            cols.append(jnp.sum(hit, axis=1, keepdims=True))
        col = jnp.concatenate(cols, axis=0).astype(jnp.int32)
        hot = (col == iota((groups * cap, shard), 1)).astype(f32).astype(bf16)
        got = mm(hot, table_ref[f]).astype(bf16)
        out_ref[:, f * cap : (f + 1) * cap, :] = got.reshape(groups, cap, got.shape[1])


def slots_body(rem_ref, quot_ref, label_ref, table_ref, pick_ref, q_ref, cols_ref, code_ref, *, shard, cap, groups, high):
    feats, tok = rem_ref.shape
    width = table_ref.shape[2]
    pad = jnp.zeros((8 - 2 * feats - 1, tok), f32)
    cols = jnp.concatenate(
        [rem_ref[...].astype(f32), quot_ref[...].astype(f32), label_ref[...].astype(f32), pad], axis=0
    ).T
    cols_ref[...] = cols
    earlier = (iota((tok, tok), 1) < iota((tok, tok), 0)).astype(f32)
    owner = iota((tok, 128), 1)
    low = (owner * shard).astype(f32)
    lane = iota((tok, code_ref.shape[2]), 1)
    codes = [[0.0, 0.0] for _ in range(groups)]
    for f in range(feats):
        ids = cols[:, f : f + 1]
        mine = ((ids >= low) & (ids < low + shard) & (owner < groups)).astype(f32)
        rank = mm(earlier, mine)
        slot = jnp.sum(mine * (rank + (owner * cap).astype(f32)), axis=1, keepdims=True)
        slot = slot.astype(jnp.int32)
        for k in range(groups):
            hit = (slot + (f - k) * cap == lane) & (mine[:, k : k + 1] > 0.0)
            local = ids - k * shard
            coarse = jnp.floor(local * (1.0 / high))
            for i, value in enumerate((coarse, local - coarse * high)):
                codes[k][i] = codes[k][i] + jnp.sum(jnp.where(hit, value, 0.0), axis=0, keepdims=True)
        pick_ref[f] = (slot == iota((tok, groups * cap), 1)).astype(f32).astype(bf16)
        quot = cols[:, feats + f : feats + f + 1].astype(jnp.int32)
        onehot = (quot == iota((tok, table_ref.shape[1]), 1)).astype(f32).astype(bf16)
        q_ref[:, f * width : (f + 1) * width] = mm(onehot, table_ref[f])
    which = iota(code_ref.shape[1:], 0)
    for k in range(groups):
        code_ref[k] = jnp.where(which == 0, codes[k][0], jnp.where(which == 1, codes[k][1], 0.0)).astype(bf16)


def step_body(
    core_ref, recv_ref, pick_ref, q_ref, cols_ref, code_ref, w1_ref, b1_ref, w2_ref, b2_ref,
    loss_ref, rem_ref, keep_ref, send_ref, tiny_ref,
    joined_s, qgrad_s, onehot_s, *, cap, parts,
):
    groups = recv_ref.shape[0]
    feats, tok, _ = pick_ref.shape
    width = recv_ref.shape[2]
    hid = w1_ref.shape[1]
    rows = onehot_s.shape[2]
    core = core_ref[0]
    preact = jnp.broadcast_to(b1_ref[...], (tok, hid))
    total = jnp.zeros((tok, hid), f32)
    rem_parts = []
    for f in range(feats):
        got = recv_ref[:, f * cap : (f + 1) * cap, :].reshape(groups * cap, width)
        rem = mm(pick_ref[f], got)
        rem_parts.append(rem)
        joined = (q_ref[:, f * width : (f + 1) * width] * rem).astype(bf16)
        joined_s[f] = joined
        total = total + mm(joined, w1_ref[f * width : (f + 1) * width, :])
        quot = cols_ref[:, feats + f : feats + f + 1].astype(jnp.int32)
        onehot_s[f] = (quot == iota((tok, rows), 1)).astype(f32)
    preact = total + preact
    sig = jax.nn.sigmoid(preact)
    hidden = (preact * sig).astype(bf16).astype(f32)
    w2_row = w2_ref[...].astype(f32)
    logits = jnp.sum(hidden * w2_row, axis=1, keepdims=True) + b2_ref[0]
    target = cols_ref[:, 2 * feats : 2 * feats + 1]
    loss = jnp.maximum(logits, 0.0) + jnp.log1p(jnp.exp(-jnp.abs(logits))) - target * logits
    loss_ref[...] = jnp.broadcast_to(loss, (tok, tok)).T[0:1, :]
    dlogits = jax.nn.sigmoid(logits) - target
    slopes = sig * (1.0 + preact * (1.0 - sig))
    dpre = dlogits * w2_row * slopes
    tiny_ref[0:1, :] = jnp.sum(dpre, axis=0, keepdims=True)
    tiny_ref[1:2, :] = jnp.sum(dlogits * hidden, axis=0, keepdims=True)
    tiny_ref[2:3, :] = jnp.sum(jnp.broadcast_to(dlogits, (tok, hid)), axis=0, keepdims=True)
    tiny_ref[3:TINY, :] = jnp.zeros((TINY - 3, hid), f32)
    rounded = dpre.astype(bf16)
    piece = width // parts
    packed = []
    for f in range(feats):
        djoined = mm(rounded, w1_ref[f * width : (f + 1) * width, :], ((1,), (1,)))
        qgrad_s[f] = djoined * rem_parts[f]
        rem_grad = (djoined * q_ref[:, f * width : (f + 1) * width]).astype(bf16)
        packed.append(mm(pick_ref[f], rem_grad, ((0,), (0,))))
    for d in range(parts):
        both = [p[:, d * piece : (d + 1) * piece] for p in packed]
        both = jnp.concatenate(both, axis=1).astype(bf16)
        rem_ref[d, :, 0:cap, :] = both.reshape(groups, cap, feats * piece)
        rem_ref[d, :, cap:, :] = code_ref[...]
    for which, out_ref in ((1 - core, send_ref), (core, keep_ref)):
        grad_w = mm(joined_s[which], rounded, ((0,), (0,)))
        grad_q = mm(onehot_s[which], qgrad_s[which], ((0,), (0,)), precision=lax.Precision.HIGHEST)
        out_ref[0:width, :] = grad_w.astype(out_ref.dtype)
        out_ref[width : width + rows, :] = grad_q.astype(out_ref.dtype)
    send_ref[width + rows :, :] = pack_tiny(tiny_ref[0:1, :], tiny_ref[1:2, :], tiny_ref[2:3, :])


def pair_body(me_ref, keep_ref, tiny_ref, recv_ref, *refs):
    out_refs, all_s = refs[:-1], refs[-1]
    parts, rows = all_s.shape[0], all_s.shape[1] - TINY
    me = me_ref[0]
    got = unpack_tiny(recv_ref[parts * rows :, :])
    tiny = pack_tiny(*(tiny_ref[i : i + 1, :] + got[i] for i in range(3)))
    for p in range(parts):
        at = slice(p * rows, (p + 1) * rows)
        all_s[p, 0:rows, :] = (keep_ref[at, :] + recv_ref[at, :].astype(f32)).astype(bf16)
        all_s[p, rows:, :] = tiny
    for k in range(parts):
        out_refs[k][...] = all_s[me ^ k]


def plane_body(*refs):
    recv_refs, out_ref = refs[:-1], refs[-1]
    rows = out_ref.shape[0] - TINY
    out_ref[0:rows, :] = tree_sum(r[0:rows, :].astype(f32) for r in recv_refs).astype(bf16)
    tiny = [unpack_tiny(r[rows:, :]) for r in recv_refs]
    out_ref[rows:, :] = pack_tiny(*(tree_sum(t[i] for t in tiny) for i in range(3)))


def add_body(mine_ref, recv_ref, out_ref):
    rows = mine_ref.shape[0] - TINY
    out_ref[0:rows, :] = (mine_ref[0:rows, :].astype(f32) + recv_ref[0:rows, :].astype(f32)).astype(bf16)
    mine, got = unpack_tiny(mine_ref[rows:, :]), unpack_tiny(recv_ref[rows:, :])
    out_ref[rows:, :] = pack_tiny(*(a + b for a, b in zip(mine, got)))


def last_body(mine_ref, recv_ref, out_ref, b1_ref, w2_ref, b2_ref):
    rows = mine_ref.shape[0] - TINY
    out_ref[...] = (mine_ref[0:rows, :].astype(f32) + recv_ref[0:rows, :].astype(f32)).astype(bf16)
    mine, got = unpack_tiny(mine_ref[rows:, :]), unpack_tiny(recv_ref[rows:, :])
    b1_ref[...] = mine[0] + got[0]
    w2_ref[...] = mine[1] + got[1]
    b2_ref[...] = (mine[2] + got[2])[:, 0:1]


def final_body(core_ref, mine_ref, other_ref, w1_ref, quot_ref):
    core = core_ref[0]
    width = w1_ref.shape[1]
    for which, ref in ((core, mine_ref), (1 - core, other_ref)):
        w1_ref[which] = ref[0:width, :].astype(f32)
        quot_ref[which] = ref[width:, :].astype(f32)


def scatter_body(grads_ref, out_ref, e_s, *, high, cap):
    feats, piece, shard = out_ref.shape
    steps = shard // high
    chunk = e_s.shape[1]
    total = grads_ref.shape[0]
    some = chunk // cap
    accs = [jnp.zeros((steps * piece, high), f32) for _ in range(feats)]
    for at in range(0, total, some):
        values = grads_ref[at : at + some, 0:cap, :].astype(f32).reshape(chunk, feats * piece).T
        codes = [grads_ref[at + i, cap:, :].astype(f32) for i in range(some)]
        for f in range(feats):
            code = jnp.concatenate([c[:, f * cap : (f + 1) * cap] for c in codes], axis=1).astype(jnp.int32)
            hot = (iota((high, chunk), 0) == code[1:2, :]).astype(f32).astype(bf16)
            mine = values[f * piece : (f + 1) * piece, :]
            for s in range(steps):
                e_s[s * piece : (s + 1) * piece, :] = jnp.where(code[0:1, :] == s, mine, 0.0).astype(bf16)
            accs[f] = accs[f] + mm(e_s[...], hot, ((1,), (1,)))
    for f in range(feats):
        for s in range(steps):
            out_ref[f, :, s * high : (s + 1) * high] = accs[f][s * piece : (s + 1) * piece, :]


def on_device(quot_ids, rem_ids, labels, quot_table, rem_table, w1, b1, w2, b2, *, sizes):
    nz, ny, nx, nc = sizes
    dp, grp = nz * ny, nx * nc
    tok, feats = rem_ids.shape
    shard, width = rem_table.shape[1], rem_table.shape[2]
    rows_q = quot_table.shape[1]
    hid = w1.shape[1]
    cap = 2 * tok // grp
    piece = width // dp
    struct = jax.ShapeDtypeStruct
    core = lax.axis_index("c")[None]
    me = (lax.axis_index("x") * nc + lax.axis_index("c"))[None]

    ids_all = lax.all_gather(rem_ids.T.reshape(-1), ("x", "c"), tiled=True).reshape(grp * feats, tok)
    picked = call(
        functools.partial(fetch_body, cap=cap), struct((grp, feats * cap, width), bf16),
        (me, ids_all, rem_table), [SM, VM, VM],
    )
    recv = lax.all_to_all(picked, ("x", "c"), 0, 0, tiled=True)

    pick, q_rows, cols, codes = call(
        functools.partial(slots_body, shard=shard, cap=cap, groups=grp, high=HIGH),
        (
            struct((feats, tok, grp * cap), bf16), struct((tok, feats * width), f32), struct((tok, 8), f32),
            struct((grp, TINY, feats * piece), bf16),
        ),
        (rem_ids.T, quot_ids.T, labels[None, :], quot_table),
        [VM] * 4,
    )
    half = width + rows_q
    loss, rem_send, keep, send, tiny = call(
        functools.partial(step_body, cap=cap, parts=dp),
        (
            struct((1, tok), f32),
            struct((dp, grp, cap + TINY, feats * piece), bf16),
            struct((half, hid), f32),
            struct((half + TINY, hid), bf16),
            struct((TINY, hid), f32),
        ),
        (core, recv, pick, q_rows, cols, codes, w1, b1[None, :], w2[None, :], b2),
        [SM] + [VM] * 8 + [SM],
        [
            pltpu.VMEM((feats, tok, width), bf16),
            pltpu.VMEM((feats, tok, width), f32),
            pltpu.VMEM((feats, tok, rows_q), f32),
        ],
    )
    swap = [(i, i ^ 1) for i in range(nc)]
    other = lax.ppermute(send, "c", swap)
    rem_send = rem_send.reshape(dp * grp, cap + TINY, feats * piece)
    rem_got = lax.all_to_all(rem_send, ("z", "y", "x", "c"), 0, 0, tiled=True)

    plane = ny * nx
    part = half // plane
    spot = (lax.axis_index("y") * nx + lax.axis_index("x"))[None]
    wire = struct((part + TINY, hid), bf16)
    blocks = call(
        pair_body, (wire,) * plane, (spot, keep, tiny, other), [SM] + [VM] * 3,
        [pltpu.VMEM((plane, part + TINY, hid), bf16)],
    )
    got = [
        lax.ppermute(blocks[k], ("y", "x"), [(i, i ^ k) for i in range(plane)]) for k in range(1, plane)
    ]
    block = call(plane_body, wire, (blocks[0], *got), [VM] * plane)
    step = 1
    while step < nz:
        got = lax.ppermute(block, "z", [(i, i ^ step) for i in range(nz)])
        step *= 2
        if step < nz:
            block = call(add_body, wire, (block, got), [VM] * 2)
        else:
            row = struct((1, hid), f32)
            block, sum_b1, sum_w2, sum_b2 = call(
                last_body, (struct((part, hid), bf16), row, row, struct((1, 1), f32)), (block, got), [VM] * 2
            )

    grad_rem = call(
        functools.partial(scatter_body, high=HIGH, cap=cap),
        struct((feats, piece, shard), f32),
        (rem_got,),
        [VM],
        [pltpu.VMEM((shard // HIGH * piece, 512), bf16)],
    )
    block = lax.all_gather(block, ("y", "x"), tiled=True)
    other = lax.ppermute(block, "c", swap)
    grad_w1, grad_quot = call(
        final_body,
        (struct((feats, width, hid), f32), struct((feats, rows_q, width), f32)),
        (core, block, other),
        [SM, VM, VM],
    )
    return (
        loss.reshape(tok), grad_rem.transpose(0, 2, 1), grad_quot, grad_w1.reshape(feats * width, hid),
        sum_b1.reshape(hid), sum_w2.reshape(hid), sum_b2.reshape(1),
    )


def solution(mesh):
    dp, grp = mesh.shape["dp"], mesh.shape["grp"]
    sizes = (dp // 2, 2, grp // 2, 2)
    fine = Mesh(mesh.devices.reshape(sizes), ("z", "y", "x", "c"))
    every, group, data = ("z", "y", "x", "c"), ("x", "c"), ("z", "y")
    placed = (P(every, None), P(every, None), P(every), P(), P(None, group, None), P(), P(), P(), P())
    return jax.shard_map(
        functools.partial(on_device, sizes=sizes),
        mesh=fine,
        in_specs=placed,
        out_specs=(P(every), P(None, group, data), P(), P(), P(), P(), P()),
        check_vma=False,
    )
```

```python
import functools

import jax
import jax.numpy as jnp
from jax import lax
from jax.experimental import pallas as pl
from jax.experimental.pallas import tpu as pltpu
from jax.sharding import Mesh, PartitionSpec as P


f32 = jnp.float32
bf16 = jnp.bfloat16
VM = pl.BlockSpec(memory_space=pltpu.VMEM)
SM = pl.BlockSpec(memory_space=pltpu.SMEM)
TINY = 8
HIGH = 256


def iota(shape, dim):
    return lax.broadcasted_iota(jnp.int32, shape, dim)


def mm(a, b, dims=((1,), (0,)), **kw):
    return lax.dot_general(a, b, (dims, ((), ())), preferred_element_type=f32, **kw)


def call(body, outs, args, in_specs, scratch=()):
    multi = isinstance(outs, (tuple, list))
    return pl.pallas_call(
        body,
        out_shape=outs,
        in_specs=in_specs,
        out_specs=tuple(VM for _ in outs) if multi else VM,
        scratch_shapes=list(scratch),
    )(*args)


def tree_sum(parts):
    parts = list(parts)
    while len(parts) > 1:
        parts = [a + b for a, b in zip(parts[::2], parts[1::2])]
    return parts[0]


def pack_tiny(b1_row, w2_row, b2_row):
    width = b1_row.shape[1]
    which = iota((TINY, width), 0)
    out = jnp.zeros((TINY, width), f32)
    at = 0
    for row in (b1_row, w2_row, b2_row):
        rest = row
        for _ in range(3):
            head = rest.astype(bf16).astype(f32)
            if at < TINY:
                out = jnp.where(which == at, head, out)
            rest = rest - head
            at += 1
        if at == 6:
            break
    lane = iota((1, width), 1)
    rest = b2_row
    last = jnp.zeros((1, width), f32)
    for piece in range(3):
        head = rest.astype(bf16).astype(f32)
        last = jnp.where(lane == piece, head, last)
        rest = rest - head
    out = jnp.where(which == 6, last, out)
    return out.astype(bf16)


def unpack_tiny(block):
    block = block.astype(f32)
    b1_row = block[0:1] + block[1:2] + block[2:3]
    w2_row = block[3:4] + block[4:5] + block[5:6]
    b2_row = block[6:7, 0:1] + block[6:7, 1:2] + block[6:7, 2:3]
    return b1_row, w2_row, jnp.broadcast_to(b2_row, b1_row.shape)


def fetch_body(me_ref, ids_ref, table_ref, *refs, cap):
    out_refs, (key_s, value_s, table_s, sems) = refs[:-4], refs[-4:]
    n_rows, tok = ids_ref.shape
    feats, shard, width = table_ref.shape
    chunks, chunk = table_s.shape[1], table_s.shape[2]
    groups = n_rows // feats
    copies = [
        [
            pltpu.make_async_copy(
                table_ref.at[f, pl.ds(c * chunk, chunk), :], table_s.at[f, c], sems.at[f, c]
            )
            for c in range(chunks)
        ]
        for f in range(feats)
    ]
    for row in copies:
        for copy in row:
            copy.start()
    me = me_ref[0]
    local = ids_ref[...] - me * shard
    mine = (local >= 0) & (local < shard)
    before = (iota((tok, tok), 0) < iota((tok, tok), 1)).astype(f32)
    key_s[...] = jnp.where(mine, mm(mine.astype(f32), before), -1.0).astype(jnp.int32)
    value_s[...] = local.astype(f32)
    slot = iota((cap, tok), 0)
    for f in range(feats):
        cols = []
        for k in range(groups):
            at = (me ^ k) * feats + f
            hit = jnp.where(key_s[pl.ds(at, 1), :] == slot, value_s[pl.ds(at, 1), :], 0.0)
            cols.append(jnp.sum(hit, axis=1, keepdims=True))
        col = jnp.concatenate(cols, axis=0).astype(jnp.int32)
        got = jnp.zeros((groups * cap, width), f32)
        for c in range(chunks):
            hot = (col - c * chunk == iota((groups * cap, chunk), 1)).astype(f32).astype(bf16)
            copies[f][c].wait()
            got = got + mm(hot, table_s[f, c])
        for k in range(groups):
            out_refs[k][f * cap : (f + 1) * cap, :] = got[k * cap : (k + 1) * cap].astype(bf16)


def slots_body(me_ref, rem_ref, quot_ref, label_ref, table_ref, pick_ref, q_ref, cols_ref, code_ref, *, shard, cap, groups, high):
    feats, tok = rem_ref.shape
    width = table_ref.shape[2]
    pad = jnp.zeros((8 - 2 * feats - 1, tok), f32)
    cols = jnp.concatenate(
        [rem_ref[...].astype(f32), quot_ref[...].astype(f32), label_ref[...].astype(f32), pad], axis=0
    ).T
    cols_ref[...] = cols
    earlier = (iota((tok, tok), 1) < iota((tok, tok), 0)).astype(f32)
    owner = iota((tok, 128), 1)
    me = me_ref[0]
    turn = iota((tok, 128), 1) ^ me
    low = (turn * shard).astype(f32)
    lane = iota((tok, code_ref.shape[2]), 1)
    codes = [[0.0, 0.0] for _ in range(groups)]
    for f in range(feats):
        ids = cols[:, f : f + 1]
        mine = ((ids >= low) & (ids < low + shard) & (owner < groups)).astype(f32)
        rank = mm(earlier, mine)
        slot = jnp.sum(mine * (rank + (owner * cap).astype(f32)), axis=1, keepdims=True)
        slot = slot.astype(jnp.int32)
        for k in range(groups):
            hit = (slot + (f - k) * cap == lane) & (mine[:, k : k + 1] > 0.0)
            local = ids - ((me ^ k) * shard).astype(f32)
            coarse = jnp.floor(local * (1.0 / high))
            for i, value in enumerate((coarse, local - coarse * high)):
                codes[k][i] = codes[k][i] + jnp.sum(jnp.where(hit, value, 0.0), axis=0, keepdims=True)
        pick_ref[f] = (slot == iota((tok, groups * cap), 1)).astype(f32).astype(bf16)
        quot = cols[:, feats + f : feats + f + 1].astype(jnp.int32)
        onehot = (quot == iota((tok, table_ref.shape[1]), 1)).astype(f32).astype(bf16)
        q_ref[:, f * width : (f + 1) * width] = mm(onehot, table_ref[f])
    which = iota(code_ref.shape[1:], 0)
    for k in range(groups):
        code_ref[k] = jnp.where(which == 0, codes[k][0], jnp.where(which == 1, codes[k][1], 0.0)).astype(bf16)


def store_parts(out_ref, start, value):
    part = out_ref.part
    at = 0
    while at < value.shape[0]:
        p, inner = divmod(start + at, part)
        many = min(part - inner, value.shape[0] - at)
        out_ref.ref[p, inner : inner + many, :] = value[at : at + many].astype(out_ref.ref.dtype)
        at += many


class Parts:
    def __init__(self, ref, part):
        self.ref, self.part = ref, part


def step_body(spot_ref, pick_ref, q_ref, cols_ref, code_ref, w1_ref, b1_ref, w2_ref, b2_ref, *refs, cap, parts, part):
    loss_ref, rem_ref, keep_ref, send_ref, joined_s, qgrad_s, onehot_s, tiny_ref = refs[-8:]
    recv_refs = refs[:-8]
    feats, tok, _ = pick_ref.shape
    groups = len(recv_refs)
    width = recv_refs[0].shape[1]
    hid = w1_ref.shape[1]
    rows = onehot_s.shape[2]
    core, me = spot_ref[0], spot_ref[1]
    preact = jnp.broadcast_to(b1_ref[...], (tok, hid))
    total = jnp.zeros((tok, hid), f32)
    rem_parts = []
    for f in range(feats):
        got = jnp.concatenate([r[f * cap : (f + 1) * cap, :] for r in recv_refs], axis=0)
        rem = mm(pick_ref[f], got)
        rem_parts.append(rem)
        joined = (q_ref[:, f * width : (f + 1) * width] * rem).astype(bf16)
        joined_s[f] = joined
        total = total + mm(joined, w1_ref[f * width : (f + 1) * width, :])
        quot = cols_ref[:, feats + f : feats + f + 1].astype(jnp.int32)
        onehot_s[f] = (quot == iota((tok, rows), 1)).astype(f32)
    preact = total + preact
    sig = jax.nn.sigmoid(preact)
    hidden = (preact * sig).astype(bf16).astype(f32)
    w2_row = w2_ref[...].astype(f32)
    logits = jnp.sum(hidden * w2_row, axis=1, keepdims=True) + b2_ref[0]
    target = cols_ref[:, 2 * feats : 2 * feats + 1]
    loss = jnp.maximum(logits, 0.0) + jnp.log1p(jnp.exp(-jnp.abs(logits))) - target * logits
    loss_ref[...] = jnp.broadcast_to(loss, (tok, tok)).T[0:1, :]
    dlogits = jax.nn.sigmoid(logits) - target
    slopes = sig * (1.0 + preact * (1.0 - sig))
    dpre = dlogits * w2_row * slopes
    tiny_ref[0:1, :] = jnp.sum(dpre, axis=0, keepdims=True)
    tiny_ref[1:2, :] = jnp.sum(dlogits * hidden, axis=0, keepdims=True)
    tiny_ref[2:3, :] = jnp.sum(jnp.broadcast_to(dlogits, (tok, hid)), axis=0, keepdims=True)
    tiny_ref[3:TINY, :] = jnp.zeros((TINY - 3, hid), f32)
    rounded = dpre.astype(bf16)
    piece = width // parts
    packed = []
    for f in range(feats):
        djoined = mm(rounded, w1_ref[f * width : (f + 1) * width, :], ((1,), (1,)))
        qgrad_s[f] = djoined * rem_parts[f]
        rem_grad = (djoined * q_ref[:, f * width : (f + 1) * width]).astype(bf16)
        packed.append(mm(pick_ref[f], rem_grad, ((0,), (0,))))
    for d in range(parts):
        both = [p[:, d * piece : (d + 1) * piece] for p in packed]
        both = jnp.concatenate(both, axis=1).astype(bf16)
        for k in range(groups):
            rem_ref[d, me ^ k, 0:cap, :] = both[k * cap : (k + 1) * cap]
            rem_ref[d, me ^ k, cap:, :] = code_ref[k]
    for which, out_ref in ((1 - core, send_ref), (core, keep_ref)):
        grad_w = mm(joined_s[which], rounded, ((0,), (0,)))
        grad_q = mm(onehot_s[which], qgrad_s[which], ((0,), (0,)), precision=lax.Precision.HIGHEST)
        store_parts(Parts(out_ref, part), 0, grad_w)
        store_parts(Parts(out_ref, part), width, grad_q)
    tiny = pack_tiny(tiny_ref[0:1, :], tiny_ref[1:2, :], tiny_ref[2:3, :])
    for p in range(send_ref.shape[0]):
        send_ref[p, part:, :] = tiny


def plane_body(*refs):
    recv_refs, out_ref = refs[:-1], refs[-1]
    rows = out_ref.shape[0] - TINY
    out_ref[0:rows, :] = tree_sum(r[0:rows, :].astype(f32) for r in recv_refs).astype(bf16)
    tiny = []
    for r in recv_refs:
        mine, other = unpack_tiny(r[rows : rows + TINY, :]), unpack_tiny(r[rows + TINY :, :])
        tiny.append([a + b for a, b in zip(mine, other)])
    out_ref[rows:, :] = pack_tiny(*(tree_sum(t[i] for t in tiny) for i in range(3)))


def last_body(rows_ref, b1_ref, w2_ref, b2_ref):
    tiny = [unpack_tiny(rows_ref[at : at + TINY, :]) for at in range(0, rows_ref.shape[0], TINY)]
    b1_ref[...] = tree_sum(t[0] for t in tiny)
    w2_ref[...] = tree_sum(t[1] for t in tiny)
    b2_ref[...] = tree_sum(t[2] for t in tiny)[:, 0:1]


def scatter_body(grads_ref, out_ref, e_s, *, high, cap):
    feats, piece, shard = out_ref.shape
    steps = shard // high
    chunk = e_s.shape[1]
    total = grads_ref.shape[0]
    some = chunk // cap
    accs = [jnp.zeros((steps * piece, high), f32) for _ in range(feats)]
    for at in range(0, total, some):
        values = grads_ref[at : at + some, 0:cap, :].astype(f32).reshape(chunk, feats * piece).T
        codes = [grads_ref[at + i, cap:, :].astype(f32) for i in range(some)]
        for f in range(feats):
            code = jnp.concatenate([c[:, f * cap : (f + 1) * cap] for c in codes], axis=1).astype(jnp.int32)
            hot = (iota((high, chunk), 0) == code[1:2, :]).astype(f32).astype(bf16)
            mine = values[f * piece : (f + 1) * piece, :]
            for s in range(steps):
                e_s[s * piece : (s + 1) * piece, :] = jnp.where(code[0:1, :] == s, mine, 0.0).astype(bf16)
            accs[f] = accs[f] + mm(e_s[...], hot, ((1,), (1,)))
    for f in range(feats):
        for s in range(steps):
            out_ref[f, :, s * high : (s + 1) * high] = accs[f][s * piece : (s + 1) * piece, :]


def on_device(quot_ids, rem_ids, labels, quot_table, rem_table, w1, b1, w2, b2, *, sizes):
    nz, ny, nx, nc = sizes
    dp, grp = nz * ny, nx * nc
    tok, feats = rem_ids.shape
    shard, width = rem_table.shape[1], rem_table.shape[2]
    rows_q = quot_table.shape[1]
    hid = w1.shape[1]
    cap = 2 * tok // grp
    piece = width // dp
    struct = jax.ShapeDtypeStruct
    core = lax.axis_index("c")[None]
    me = (lax.axis_index("x") * nc + lax.axis_index("c"))[None]

    ids_all = lax.all_gather(rem_ids.T.reshape(-1), ("x", "c"), tiled=True).reshape(grp * feats, tok)
    picked = call(
        functools.partial(fetch_body, cap=cap),
        (struct((feats * cap, width), bf16),) * grp,
        (me, ids_all, rem_table),
        [SM, VM, pl.BlockSpec(memory_space=pl.ANY)],
        [
            pltpu.VMEM((grp * feats, tok), jnp.int32), pltpu.VMEM((grp * feats, tok), f32),
            pltpu.VMEM((feats, 4, shard // 4, width), bf16), pltpu.SemaphoreType.DMA((feats, 4)),
        ],
    )
    recv = [picked[0]] + [lax.ppermute(picked[k], ("x", "c"), [(i, i ^ k) for i in range(grp)]) for k in range(1, grp)]

    slots = call(
        functools.partial(slots_body, shard=shard, cap=cap, groups=grp, high=HIGH),
        (
            struct((feats, tok, grp * cap), bf16), struct((tok, feats * width), f32), struct((tok, 8), f32),
            struct((grp, TINY, feats * piece), bf16),
        ),
        (me, rem_ids.T, quot_ids.T, labels[None, :], quot_table),
        [SM] + [VM] * 4,
    )
    pick, q_rows, cols, codes = slots

    half = width + rows_q
    plane = ny * nx
    part = half // plane
    loss, rem_send, keep, send = call(
        functools.partial(step_body, cap=cap, parts=dp, part=part),
        (
            struct((1, tok), f32),
            struct((dp, grp, cap + TINY, feats * piece), bf16),
            struct((plane, part, hid), f32),
            struct((plane, part + TINY, hid), bf16),
        ),
        (
            jnp.concatenate([core, me]), pick, q_rows, cols, codes, w1, b1[None, :], w2[None, :], b2, *recv,
        ),
        [SM] + [VM] * 7 + [SM] + [VM] * len(recv),
        [
            pltpu.VMEM((feats, tok, width), bf16),
            pltpu.VMEM((feats, tok, width), f32),
            pltpu.VMEM((feats, tok, rows_q), f32),
            pltpu.VMEM((TINY, hid), f32),
        ],
    )
    swap = [(i, i ^ 1) for i in range(nc)]
    other = lax.ppermute(send, "c", swap)
    rem_send = rem_send.reshape(dp * grp, cap + TINY, feats * piece)
    rem_got = lax.all_to_all(rem_send, ("z", "y", "x", "c"), 0, 0, tiled=True)

    spot = lax.axis_index("y") * nx + lax.axis_index("x")
    wire = struct((part + TINY, hid), bf16)
    blocks = []
    for k in range(plane):
        kept = lax.dynamic_index_in_dim(keep, spot ^ k, 0, keepdims=False)
        came = lax.dynamic_index_in_dim(other, spot ^ k, 0, keepdims=False)
        main = (kept + came[:part].astype(f32)).astype(bf16)
        blocks.append(jnp.concatenate([main, send[0, part:], other[0, part:]]))
    got = [
        lax.ppermute(blocks[k], ("y", "x"), [(i, i ^ k) for i in range(plane)]) for k in range(1, plane)
    ]
    block = call(plane_body, wire, (blocks[0], *got), [VM] * plane)
    main, tiny_rows = block[:part], block[part:]
    step = 1
    while step < nz:
        got = lax.ppermute(block, "z", [(i, i ^ step) for i in range(nz)])
        step *= 2
        main = (main.astype(f32) + got[:part].astype(f32)).astype(bf16)
        tiny_rows = jnp.concatenate([tiny_rows, got[part:]])
        if step < nz:
            block = lax.optimization_barrier(jnp.concatenate([main, tiny_rows]))
            main, tiny_rows = block[:part], block[part:]
    main = lax.optimization_barrier(main)
    row = struct((1, hid), f32)
    sum_b1, sum_w2, sum_b2 = call(last_body, (row, row, struct((1, 1), f32)), (tiny_rows,), [VM])

    grad_rem = call(
        functools.partial(scatter_body, high=HIGH, cap=cap),
        struct((feats, piece, shard), f32),
        (rem_got,),
        [VM],
        [pltpu.VMEM((shard // HIGH * piece, 512), bf16)],
    )
    block = lax.all_gather(main, ("y", "x"), tiled=True)
    other = lax.ppermute(block, "c", swap)
    first, second = jnp.where(core == 0, block, other), jnp.where(core == 0, other, block)
    grad_w1 = jnp.stack([first[:width], second[:width]]).astype(f32)
    grad_quot = jnp.stack([first[width:], second[width:]]).astype(f32)
    return (
        loss.reshape(tok), grad_rem.transpose(0, 2, 1), grad_quot, grad_w1.reshape(feats * width, hid),
        sum_b1.reshape(hid), sum_w2.reshape(hid), sum_b2.reshape(1),
    )


def solution(mesh):
    dp, grp = mesh.shape["dp"], mesh.shape["grp"]
    sizes = (dp // 2, 2, grp // 2, 2)
    fine = Mesh(mesh.devices.reshape(sizes), ("z", "y", "x", "c"))
    every, group, data = ("z", "y", "x", "c"), ("x", "c"), ("z", "y")
    placed = (P(every, None), P(every, None), P(every), P(), P(None, group, None), P(), P(), P(), P())
    return jax.shard_map(
        functools.partial(on_device, sizes=sizes),
        mesh=fine,
        in_specs=placed,
        out_specs=(P(every), P(None, group, data), P(), P(), P(), P(), P()),
        check_vma=False,
    )
```

```python
import functools

import jax
import jax.numpy as jnp
from jax import lax
from jax.experimental import pallas as pl
from jax.experimental.pallas import tpu as pltpu
from jax.sharding import Mesh, PartitionSpec as P


f32 = jnp.float32
bf16 = jnp.bfloat16
VM = pl.BlockSpec(memory_space=pltpu.VMEM)
SM = pl.BlockSpec(memory_space=pltpu.SMEM)
TINY = 8
HIGH = 256


def iota(shape, dim):
    return lax.broadcasted_iota(jnp.int32, shape, dim)


def mm(a, b, dims=((1,), (0,)), **kw):
    return lax.dot_general(a, b, (dims, ((), ())), preferred_element_type=f32, **kw)


def call(body, outs, args, in_specs, scratch=()):
    multi = isinstance(outs, (tuple, list))
    return pl.pallas_call(
        body,
        out_shape=outs,
        in_specs=in_specs,
        out_specs=tuple(VM for _ in outs) if multi else VM,
        scratch_shapes=list(scratch),
    )(*args)


def tree_sum(parts):
    parts = list(parts)
    while len(parts) > 1:
        parts = [a + b for a, b in zip(parts[::2], parts[1::2])]
    return parts[0]


def pack_tiny(b1_row, w2_row, b2_row):
    width = b1_row.shape[1]
    which = iota((TINY, width), 0)
    out = jnp.zeros((TINY, width), f32)
    at = 0
    for row in (b1_row, w2_row, b2_row):
        rest = row
        for _ in range(3):
            head = rest.astype(bf16).astype(f32)
            if at < TINY:
                out = jnp.where(which == at, head, out)
            rest = rest - head
            at += 1
        if at == 6:
            break
    lane = iota((1, width), 1)
    rest = b2_row
    last = jnp.zeros((1, width), f32)
    for piece in range(3):
        head = rest.astype(bf16).astype(f32)
        last = jnp.where(lane == piece, head, last)
        rest = rest - head
    out = jnp.where(which == 6, last, out)
    return out.astype(bf16)


def fetch_body(me_ref, ids_ref, table_ref, *refs, cap):
    out_refs, (key_s, value_s, table_s, sems) = refs[:-4], refs[-4:]
    n_rows, tok = ids_ref.shape
    feats, shard, width = table_ref.shape
    chunks, chunk = table_s.shape[1], table_s.shape[2]
    groups = n_rows // feats
    copies = [
        [
            pltpu.make_async_copy(
                table_ref.at[f, pl.ds(c * chunk, chunk), :], table_s.at[f, c], sems.at[f, c]
            )
            for c in range(chunks)
        ]
        for f in range(feats)
    ]
    for row in copies:
        for copy in row:
            copy.start()
    me = me_ref[0]
    local = ids_ref[...] - me * shard
    mine = (local >= 0) & (local < shard)
    before = (iota((tok, tok), 0) < iota((tok, tok), 1)).astype(f32)
    key_s[...] = jnp.where(mine, mm(mine.astype(f32), before), -1.0).astype(jnp.int32)
    value_s[...] = local.astype(f32)
    slot = iota((cap, tok), 0)
    for f in range(feats):
        cols = []
        for k in range(groups):
            at = (me ^ k) * feats + f
            hit = jnp.where(key_s[pl.ds(at, 1), :] == slot, value_s[pl.ds(at, 1), :], 0.0)
            cols.append(jnp.sum(hit, axis=1, keepdims=True))
        col = jnp.concatenate(cols, axis=0).astype(jnp.int32)
        got = jnp.zeros((groups * cap, width), f32)
        for c in range(chunks):
            hot = (col - c * chunk == iota((groups * cap, chunk), 1)).astype(f32).astype(bf16)
            copies[f][c].wait()
            got = got + mm(hot, table_s[f, c])
        for k in range(groups):
            out_refs[k][f * cap : (f + 1) * cap, :] = got[k * cap : (k + 1) * cap].astype(bf16)


def slots_body(me_ref, rem_ref, quot_ref, label_ref, table_ref, pick_ref, q_ref, cols_ref, code_ref, *, shard, cap, groups, high):
    feats, tok = rem_ref.shape
    width = table_ref.shape[2]
    pad = jnp.zeros((8 - 2 * feats - 1, tok), f32)
    cols = jnp.concatenate(
        [rem_ref[...].astype(f32), quot_ref[...].astype(f32), label_ref[...].astype(f32), pad], axis=0
    ).T
    cols_ref[...] = cols
    earlier = (iota((tok, tok), 1) < iota((tok, tok), 0)).astype(f32)
    owner = iota((tok, 128), 1)
    me = me_ref[0]
    turn = iota((tok, 128), 1) ^ me
    low = (turn * shard).astype(f32)
    lane = iota((tok, code_ref.shape[2]), 1)
    codes = [[0.0, 0.0] for _ in range(groups)]
    for f in range(feats):
        ids = cols[:, f : f + 1]
        mine = ((ids >= low) & (ids < low + shard) & (owner < groups)).astype(f32)
        rank = mm(earlier, mine)
        slot = jnp.sum(mine * (rank + (owner * cap).astype(f32)), axis=1, keepdims=True)
        slot = slot.astype(jnp.int32)
        for k in range(groups):
            hit = (slot + (f - k) * cap == lane) & (mine[:, k : k + 1] > 0.0)
            local = ids - ((me ^ k) * shard).astype(f32)
            coarse = jnp.floor(local * (1.0 / high))
            for i, value in enumerate((coarse, local - coarse * high)):
                codes[k][i] = codes[k][i] + jnp.sum(jnp.where(hit, value, 0.0), axis=0, keepdims=True)
        pick_ref[f] = (slot == iota((tok, groups * cap), 1)).astype(f32).astype(bf16)
        quot = cols[:, feats + f : feats + f + 1].astype(jnp.int32)
        onehot = (quot == iota((tok, table_ref.shape[1]), 1)).astype(f32).astype(bf16)
        q_ref[:, f * width : (f + 1) * width] = mm(onehot, table_ref[f])
    which = iota(code_ref.shape[1:], 0)
    for k in range(groups):
        code_ref[k] = jnp.where(which == 0, codes[k][0], jnp.where(which == 1, codes[k][1], 0.0)).astype(bf16)


def store_parts(out_ref, start, value):
    part = out_ref.part
    at = 0
    while at < value.shape[0]:
        p, inner = divmod(start + at, part)
        many = min(part - inner, value.shape[0] - at)
        out_ref.ref[p, inner : inner + many, :] = value[at : at + many].astype(out_ref.ref.dtype)
        at += many


class Parts:
    def __init__(self, ref, part):
        self.ref, self.part = ref, part


def step_body(spot_ref, pick_ref, q_ref, cols_ref, code_ref, w1_ref, b1_ref, w2_ref, b2_ref, *refs, cap, parts, part):
    loss_ref, rem_ref, keep_ref, send_ref, joined_s, qgrad_s, onehot_s, tiny_ref = refs[-8:]
    recv_refs = refs[:-8]
    feats, tok, _ = pick_ref.shape
    groups = len(recv_refs)
    width = recv_refs[0].shape[1]
    hid = w1_ref.shape[1]
    rows = onehot_s.shape[2]
    core, me = spot_ref[0], spot_ref[1]
    preact = jnp.broadcast_to(b1_ref[...], (tok, hid))
    total = jnp.zeros((tok, hid), f32)
    rem_parts = []
    for f in range(feats):
        got = jnp.concatenate([r[f * cap : (f + 1) * cap, :] for r in recv_refs], axis=0)
        rem = mm(pick_ref[f], got)
        rem_parts.append(rem)
        joined = (q_ref[:, f * width : (f + 1) * width] * rem).astype(bf16)
        joined_s[f] = joined
        total = total + mm(joined, w1_ref[f * width : (f + 1) * width, :])
        quot = cols_ref[:, feats + f : feats + f + 1].astype(jnp.int32)
        onehot_s[f] = (quot == iota((tok, rows), 1)).astype(f32)
    preact = total + preact
    sig = jax.nn.sigmoid(preact)
    hidden = (preact * sig).astype(bf16).astype(f32)
    w2_row = w2_ref[...].astype(f32)
    logits = jnp.sum(hidden * w2_row, axis=1, keepdims=True) + b2_ref[0]
    target = cols_ref[:, 2 * feats : 2 * feats + 1]
    loss = jnp.maximum(logits, 0.0) + jnp.log1p(jnp.exp(-jnp.abs(logits))) - target * logits
    loss_ref[...] = jnp.broadcast_to(loss, (tok, tok)).T[0:1, :]
    dlogits = jax.nn.sigmoid(logits) - target
    slopes = sig * (1.0 + preact * (1.0 - sig))
    dpre = dlogits * w2_row * slopes
    tiny_ref[0:1, :] = jnp.sum(dpre, axis=0, keepdims=True)
    tiny_ref[1:2, :] = jnp.sum(dlogits * hidden, axis=0, keepdims=True)
    tiny_ref[2:3, :] = jnp.sum(jnp.broadcast_to(dlogits, (tok, hid)), axis=0, keepdims=True)
    tiny_ref[3:TINY, :] = jnp.zeros((TINY - 3, hid), f32)
    rounded = dpre.astype(bf16)
    piece = width // parts
    packed = []
    for f in range(feats):
        djoined = mm(rounded, w1_ref[f * width : (f + 1) * width, :], ((1,), (1,)))
        qgrad_s[f] = djoined * rem_parts[f]
        rem_grad = (djoined * q_ref[:, f * width : (f + 1) * width]).astype(bf16)
        packed.append(mm(pick_ref[f], rem_grad, ((0,), (0,))))
    for d in range(parts):
        both = [p[:, d * piece : (d + 1) * piece] for p in packed]
        both = jnp.concatenate(both, axis=1).astype(bf16)
        for k in range(groups):
            rem_ref[d, me ^ k, 0:cap, :] = both[k * cap : (k + 1) * cap]
            rem_ref[d, me ^ k, cap:, :] = code_ref[k]
    for which, out_ref in ((1 - core, send_ref), (core, keep_ref)):
        grad_w = mm(joined_s[which], rounded, ((0,), (0,)))
        grad_q = mm(onehot_s[which], qgrad_s[which], ((0,), (0,)), precision=lax.Precision.HIGHEST)
        store_parts(Parts(out_ref, part), 0, grad_w)
        store_parts(Parts(out_ref, part), width, grad_q)
    tiny = pack_tiny(tiny_ref[0:1, :], tiny_ref[1:2, :], tiny_ref[2:3, :])
    empty = jnp.zeros(tiny.shape, f32)
    for p in range(send_ref.shape[0]):
        keep_ref[p, part:, :] = jnp.concatenate([tiny.astype(f32), empty], axis=0)
        send_ref[p, part:, :] = jnp.concatenate([empty, tiny.astype(f32)], axis=0).astype(bf16)


def scatter_body(grads_ref, out_ref, e_s, *, high, cap):
    feats, piece, shard = out_ref.shape
    steps = shard // high
    chunk = e_s.shape[1]
    total = grads_ref.shape[0]
    some = chunk // cap
    accs = [jnp.zeros((steps * piece, high), f32) for _ in range(feats)]
    for at in range(0, total, some):
        values = grads_ref[at : at + some, 0:cap, :].astype(f32).reshape(chunk, feats * piece).T
        codes = [grads_ref[at + i, cap:, :].astype(f32) for i in range(some)]
        for f in range(feats):
            code = jnp.concatenate([c[:, f * cap : (f + 1) * cap] for c in codes], axis=1).astype(jnp.int32)
            hot = (iota((high, chunk), 0) == code[1:2, :]).astype(f32).astype(bf16)
            mine = values[f * piece : (f + 1) * piece, :]
            for s in range(steps):
                e_s[s * piece : (s + 1) * piece, :] = jnp.where(code[0:1, :] == s, mine, 0.0).astype(bf16)
            accs[f] = accs[f] + mm(e_s[...], hot, ((1,), (1,)))
    for f in range(feats):
        for s in range(steps):
            out_ref[f, :, s * high : (s + 1) * high] = accs[f][s * piece : (s + 1) * piece, :]


def on_device(quot_ids, rem_ids, labels, quot_table, rem_table, w1, b1, w2, b2, *, sizes):
    nz, ny, nx, nc = sizes
    dp, grp = nz * ny, nx * nc
    tok, feats = rem_ids.shape
    shard, width = rem_table.shape[1], rem_table.shape[2]
    rows_q = quot_table.shape[1]
    hid = w1.shape[1]
    cap = 2 * tok // grp
    piece = width // dp
    struct = jax.ShapeDtypeStruct
    core = lax.axis_index("c")[None]
    me = (lax.axis_index("x") * nc + lax.axis_index("c"))[None]

    ids_all = lax.all_gather(rem_ids.T.reshape(-1), ("x", "c"), tiled=True).reshape(grp * feats, tok)
    picked = call(
        functools.partial(fetch_body, cap=cap),
        (struct((feats * cap, width), bf16),) * grp,
        (me, ids_all, rem_table),
        [SM, VM, pl.BlockSpec(memory_space=pl.ANY)],
        [
            pltpu.VMEM((grp * feats, tok), jnp.int32), pltpu.VMEM((grp * feats, tok), f32),
            pltpu.VMEM((feats, 4, shard // 4, width), bf16), pltpu.SemaphoreType.DMA((feats, 4)),
        ],
    )
    recv = [picked[0]] + [lax.ppermute(picked[k], ("x", "c"), [(i, i ^ k) for i in range(grp)]) for k in range(1, grp)]

    slots = call(
        functools.partial(slots_body, shard=shard, cap=cap, groups=grp, high=HIGH),
        (
            struct((feats, tok, grp * cap), bf16), struct((tok, feats * width), f32), struct((tok, 8), f32),
            struct((grp, TINY, feats * piece), bf16),
        ),
        (me, rem_ids.T, quot_ids.T, labels[None, :], quot_table),
        [SM] + [VM] * 4,
    )
    pick, q_rows, cols, codes = slots

    half = width + rows_q
    plane = ny * nx
    part = half // plane
    loss, rem_send, keep, send = call(
        functools.partial(step_body, cap=cap, parts=dp, part=part),
        (
            struct((1, tok), f32),
            struct((dp, grp, cap + TINY, feats * piece), bf16),
            struct((plane, part + 2 * TINY, hid), f32),
            struct((plane, part + 2 * TINY, hid), bf16),
        ),
        (
            jnp.concatenate([core, me]), pick, q_rows, cols, codes, w1, b1[None, :], w2[None, :], b2, *recv,
        ),
        [SM] + [VM] * 7 + [SM] + [VM] * len(recv),
        [
            pltpu.VMEM((feats, tok, width), bf16),
            pltpu.VMEM((feats, tok, width), f32),
            pltpu.VMEM((feats, tok, rows_q), f32),
            pltpu.VMEM((TINY, hid), f32),
        ],
    )
    swap = [(i, i ^ 1) for i in range(nc)]
    other = lax.ppermute(send, "c", swap)
    rem_send = rem_send.reshape(dp * grp, cap + TINY, feats * piece)
    rem_got = lax.all_to_all(rem_send, ("z", "y", "x", "c"), 0, 0, tiled=True)

    spot = lax.axis_index("y") * nx + lax.axis_index("x")
    blocks = []
    for k in range(plane):
        from_keep, from_other = lax.optimization_barrier((keep, other))
        kept = lax.dynamic_index_in_dim(from_keep, spot ^ k, 0, keepdims=False)
        came = lax.dynamic_index_in_dim(from_other, spot ^ k, 0, keepdims=False)
        blocks.append((kept + came.astype(f32)).astype(bf16))
    got = [
        lax.ppermute(blocks[k], ("y", "x"), [(i, i ^ k) for i in range(plane)]) for k in range(1, plane)
    ]
    arrived = [blocks[0], *got]
    main = tree_sum(r[:part].astype(f32) for r in arrived).astype(bf16)
    main = lax.optimization_barrier(main)
    tiny = tree_sum(r[part:].astype(f32) for r in arrived)
    tiny = tiny[:TINY] + tiny[TINY:]
    step = 1
    while step < nz:
        swap_z = [(i, i ^ step) for i in range(nz)]
        got = lax.ppermute(main, "z", swap_z)
        tiny = tiny + lax.ppermute(tiny, "z", swap_z)
        main = lax.optimization_barrier((main.astype(f32) + got.astype(f32)).astype(bf16))
        step *= 2

    grad_rem = call(
        functools.partial(scatter_body, high=HIGH, cap=cap),
        struct((feats, piece, shard), f32),
        (rem_got,),
        [VM],
        [pltpu.VMEM((shard // HIGH * piece, 512), bf16)],
    )
    block = lax.all_gather(main, ("y", "x"), tiled=True)
    other = lax.ppermute(block, "c", swap)
    first, second = jnp.where(core == 0, block, other), jnp.where(core == 0, other, block)
    grad_w1 = jnp.stack([first[:width], second[:width]]).astype(f32)
    grad_quot = jnp.stack([first[width:], second[width:]]).astype(f32)
    return (
        loss.reshape(tok), grad_rem.transpose(0, 2, 1), grad_quot, grad_w1.reshape(feats * width, hid),
        tiny[0] + tiny[1] + tiny[2], tiny[3] + tiny[4] + tiny[5], jnp.sum(tiny[6, 0:3])[None],
    )


def solution(mesh):
    dp, grp = mesh.shape["dp"], mesh.shape["grp"]
    sizes = (dp // 2, 2, grp // 2, 2)
    fine = Mesh(mesh.devices.reshape(sizes), ("z", "y", "x", "c"))
    every, group, data = ("z", "y", "x", "c"), ("x", "c"), ("z", "y")
    placed = (P(every, None), P(every, None), P(every), P(), P(None, group, None), P(), P(), P(), P())
    return jax.shard_map(
        functools.partial(on_device, sizes=sizes),
        mesh=fine,
        in_specs=placed,
        out_specs=(P(every), P(None, group, data), P(), P(), P(), P(), P()),
        check_vma=False,
    )
```
